1024 devices in a mesh: section: 16 (over z), node: 8 (over x, core), local: 8 (over y).
Axes of the slice: x: 4, y: 8, z: 16, core: 2. Of those that a mesh axis runs over, the one named last changes fastest.
Arguments:
- tokens: bfloat16 [16, 6144, 7168], P('section', ('node', 'local')), may hold values from -6 to 6
- routes: int32 [16, 6144, 8], P('section', ('node', 'local')), may hold values from 0 to 383, as said below
- route_gates: float32 [16, 6144, 8], P('section', ('node', 'local')), may hold values from 0.2 to 1
- replica_table: int32 [8], replicated, may hold values from 0 to 5, as said below
- w_gate: bfloat16 [8, 7168, 1024], P('node', None, 'local')
- w_up: bfloat16 [8, 7168, 1024], P('node', None, 'local')
- w_down: bfloat16 [8, 1024, 7168], P('node', 'local')
Outputs:
- section_input: bfloat16 [16, 6144, 7168], P('section', ('node', 'local'))
The draws below stay inside these ranges and needn't reach their ends.
Inputs may be any that keep to these rules, and one draw needn't show every extreme that they name: `replica_table`: each of the experts 0 to 5 is held by one or two slots; slots that hold the same expert hold equal weights in w_gate, w_up and w_down. `routes`: each row names 8 different experts. Within the rows of one device, expert e < 6 is named by at least one row and by at most 2 times its number of slots in replica_table; in every draw some expert with one slot is named by exactly 2 rows of every device.
All inputs are finite; a program needn't handle non-finite values.
Results may differ from the reference program's by a relative error of at most 0.015.
Values may be sent and summed in bfloat16 or wider, within the bound.
No kernel may reach another device: no remote copies, remote signals or barrier semaphores. Data moves between devices by JAX's collectives and lax.ppermute only.
A program may use at most 32 MiB of HBM per device.

```python
import jax
import jax.numpy as jnp
from jax import lax

D = 7168
ROUTED_EXPERTS = 384
TOPK = 8
HID_DEV = 128
CAP = 2
TOK_DEV = 96
FFW = 1024
EXPERTS_AFLOAT = 6
TOKG = 6144
N_SECTION = 16
N_NODE = 8
N_LOCAL = 8


def replica_table_of(key):
    table_key = jax.random.fold_in(key, 7001)
    extra = N_NODE - EXPERTS_AFLOAT
    hot_experts = jax.random.permutation(jax.random.fold_in(table_key, 1), EXPERTS_AFLOAT)[:extra]
    slots = jnp.concatenate([jnp.arange(EXPERTS_AFLOAT, dtype=jnp.int32), hot_experts.astype(jnp.int32)])
    return jax.random.permutation(jax.random.fold_in(table_key, 2), slots).astype(jnp.int32)


def draw_replica_table(key, part):
    return replica_table_of(key)


def draw_routes(key, part):
    slot_table = replica_table_of(key)
    route_key = jax.random.fold_in(key, 7002)
    blocks = N_SECTION * N_NODE * N_LOCAL
    expert_ids = jnp.arange(EXPERTS_AFLOAT, dtype=jnp.int32)
    copies = jnp.sum((slot_table[None, :] == expert_ids[:, None]).astype(jnp.int32), axis=1)
    most_rows = CAP * copies
    loads = jax.random.randint(jax.random.fold_in(route_key, 1), (blocks, EXPERTS_AFLOAT), 1, most_rows[None, :] + 1)
    full_expert = jnp.argmax(copies == 1).astype(jnp.int32)
    loads = jnp.where(expert_ids[None, :] == full_expert, CAP, loads)
    order_keys = jax.random.split(jax.random.fold_in(route_key, 2), blocks * EXPERTS_AFLOAT)
    ranks = jax.vmap(lambda one_key: jnp.argsort(jax.random.permutation(one_key, TOK_DEV)))(order_keys)
    ranks = ranks.reshape(blocks, EXPERTS_AFLOAT, TOK_DEV)
    labeled_flag = ranks < loads[:, :, None]
    labeled_flag = jnp.transpose(labeled_flag, (0, 2, 1)).reshape(blocks * TOK_DEV, EXPERTS_AFLOAT)
    row_total = blocks * TOK_DEV
    noise = jax.random.randint(jax.random.fold_in(route_key, 3), (row_total, ROUTED_EXPERTS), 0, 1 << 20)
    every_expert_index = jnp.arange(ROUTED_EXPERTS, dtype=jnp.int32)
    router_logit = noise * 512 + every_expert_index[None, :]
    traveling_piece = jnp.pad(labeled_flag, ((0, 0), (0, ROUTED_EXPERTS - EXPERTS_AFLOAT)))
    router_logit = jnp.where(every_expert_index[None, :] < EXPERTS_AFLOAT, jnp.where(traveling_piece, router_logit + (1 << 29), -1), router_logit)
    unused, chosen = lax.top_k(router_logit, TOPK)
    return chosen.astype(jnp.int32).reshape(N_SECTION, TOKG, TOPK)


def slot_weights(key, salt, array_shape, fan_in):
    slot_table = replica_table_of(key)
    weight_key = jax.random.fold_in(key, salt)

    def one_slot(expert):
        return jax.random.normal(jax.random.fold_in(weight_key, expert), array_shape, jnp.float32) * fan_in ** (-0.5)
    return jax.vmap(one_slot)(slot_table).astype(jnp.bfloat16)


def draw_w_gate(key, part):
    return slot_weights(key, 7003, (D, FFW), D)


def draw_w_up(key, part):
    return slot_weights(key, 7004, (D, FFW), D)


def draw_w_down(key, part):
    return slot_weights(key, 7005, (FFW, D), FFW)


def levels(own_key, dims, cuts, least, largest):
    loudness = 1.0
    for position, shards_of in cuts:
        steps = jax.random.uniform(jax.random.fold_in(jax.random.fold_in(own_key, 6), position), (shards_of,), jnp.float32, least / len(cuts), largest / len(cuts))
        loudness = loudness * jnp.repeat(jnp.exp(steps), dims[position] // shards_of).reshape((-1,) + (1,) * (len(dims) - 1 - position))
    return loudness


def normal_values(stream_key, extent, deviation, limit, cuts=(), held_as=jnp.bfloat16):
    array = jax.random.normal(stream_key, extent, jnp.float32) * deviation
    if len(cuts) > 0:
        array = levels(stream_key, extent, cuts, -0.22, 0.18) * array
    return jnp.clip(array, min=-limit, max=limit).astype(held_as)


def setup_inputs(seed: int = 0) -> dict:
    arg_keys = jax.random.split(jax.random.key(seed), 8)
    tokens = normal_values(arg_keys[0], (N_SECTION, TOKG, D), 1.0, 6.0, ((0, 16), (1, 64)))
    routes = draw_routes(jax.random.fold_in(arg_keys[7], 71), 0)
    route_gates = jnp.clip(0.2 + 0.8 * jax.random.uniform(arg_keys[2], (N_SECTION, TOKG, TOPK), jnp.float32) ** levels(arg_keys[2], (N_SECTION, TOKG, TOPK), ((0, 16), (1, 64)), -0.2, 0.2), 0.2, 1.0)
    replica_table = draw_replica_table(jax.random.fold_in(arg_keys[7], 71), 0)
    w_gate = draw_w_gate(jax.random.fold_in(arg_keys[7], 71), 0)
    w_up = draw_w_up(jax.random.fold_in(arg_keys[7], 71), 0)
    w_down = draw_w_down(jax.random.fold_in(arg_keys[7], 71), 0)
    return dict(tokens=tokens, routes=routes, route_gates=route_gates, replica_table=replica_table, w_gate=w_gate, w_up=w_up, w_down=w_down)


def reference(tokens, routes, route_gates, replica_table, w_gate, w_up, w_down):
    most_rows = N_NODE * N_LOCAL * 2 * CAP
    row_total = tokens.shape[1]

    def one_section(section_args):
        section_rows, pick_ids, gate_vals = section_args
        accum_out = jnp.zeros((row_total, D), jnp.float32)
        for expert in range(EXPERTS_AFLOAT):
            slot_index = jnp.argmax(replica_table == expert).astype(jnp.int32)
            gate_mat = lax.dynamic_index_in_dim(w_gate, slot_index, 0, keepdims=False)
            up_mat = lax.dynamic_index_in_dim(w_up, slot_index, 0, keepdims=False)
            down_mat = lax.dynamic_index_in_dim(w_down, slot_index, 0, keepdims=False)
            is_named = pick_ids == expert
            weight = jnp.sum(jnp.where(is_named, gate_vals, 0.0), axis=1)
            has_expert = jnp.any(is_named, axis=1)
            row_index = jnp.nonzero(has_expert, size=most_rows, fill_value=row_total)[0].astype(jnp.int32)
            chosen = jnp.take(section_rows, row_index, axis=0, mode="clip")
            gate_proj = jnp.dot(chosen, gate_mat, preferred_element_type=jnp.float32)
            up_proj = jnp.dot(chosen, up_mat, preferred_element_type=jnp.float32)
            hidden = (jax.nn.silu(gate_proj) * up_proj).astype(jnp.bfloat16)
            blocks = hidden.reshape(most_rows, N_LOCAL, HID_DEV).astype(jnp.float32)
            down_blocks = down_mat.reshape(N_LOCAL, HID_DEV, D).astype(jnp.float32)
            block_pieces = jnp.einsum("rbh,bhd->rbd", blocks, down_blocks, precision=lax.Precision.HIGHEST).astype(jnp.bfloat16)
            expert_out = jnp.sum(block_pieces.astype(jnp.float32), axis=1).astype(jnp.bfloat16)
            pick_scale = jnp.take(weight, row_index, mode="clip")
            accum_out = accum_out.at[row_index].add(pick_scale[:, None] * expert_out.astype(jnp.float32), mode="drop")
        return accum_out.astype(jnp.bfloat16)

    layer_out = lax.map(one_section, (tokens, routes, route_gates))
    return jnp.concatenate([jnp.zeros_like(layer_out[:1]), layer_out[:-1]], axis=0)
```

```python
import jax
import jax.numpy as jnp
from jax import lax
from jax.sharding import PartitionSpec as P

TOPK = 8
CAP = 2


def passed_along(block, axis, distance):
    devices = range(lax.axis_size(axis))
    route = [(i - distance, i) for i in devices if i - distance in devices]
    return lax.ppermute(block, axis, route)


def routing(routes, route_gates, replica_table, n_node, tok_dev):
    experts = n_node * 3 // 4
    pick_ids = routes[0].reshape(-1)
    gate_vals = route_gates[0]
    expert_ids = jnp.arange(experts, dtype=jnp.int32)
    slot_match = replica_table[:, None] == expert_ids[None, :]
    copies = jnp.sum(slot_match.astype(jnp.int32), axis=0)
    slot_rank = jnp.cumsum(slot_match.astype(jnp.int32), axis=0) - 1
    pick_match = pick_ids[:, None] == expert_ids[None, :]
    pick_rank = jnp.cumsum(pick_match.astype(jnp.int32), axis=0) - 1
    own_rank = jnp.sum(jnp.where(pick_match, pick_rank, 0), axis=1)
    own_copies = jnp.sum(jnp.where(pick_match, copies[None, :], 0), axis=1)
    in_flight = jnp.any(pick_match, axis=1)
    safe_copies = jnp.maximum(own_copies, 1)
    replica = own_rank % safe_copies
    position = own_rank // safe_copies
    slot_hit = (
        pick_match[:, None, :]
        & slot_match[None, :, :]
        & (slot_rank[None, :, :] == replica[:, None, None])
    )
    slot_ids = jnp.arange(n_node, dtype=jnp.int32)
    slot_of = jnp.sum(jnp.where(jnp.any(slot_hit, axis=2), slot_ids[None, :], 0), axis=1)
    target = jnp.where(in_flight, slot_of * CAP + position, -1)
    buffer_ids = jnp.arange(n_node * CAP, dtype=jnp.int32)
    select = (target[None, :] == buffer_ids[:, None]).reshape(n_node * CAP, tok_dev, TOPK)
    dispatch = jnp.any(select, axis=2).astype(jnp.bfloat16)
    combine = jnp.sum(jnp.where(select, gate_vals[None, :, :], 0.0), axis=2)
    return dispatch, combine


def shards(tokens, routes, route_gates, replica_table, w_gate, w_up, w_down):
    n_node = lax.axis_size("node")
    n_local = lax.axis_size("local")
    rows_in = tokens[0]
    tok_dev, width = rows_in.shape
    rows_dev = n_node * CAP
    dispatch, combine = routing(routes, route_gates, replica_table, n_node, tok_dev)
    weights = passed_along(combine, "section", 1)
    outgoing = jnp.dot(dispatch, rows_in, preferred_element_type=jnp.float32).astype(jnp.bfloat16)
    arrived = lax.all_to_all(
        outgoing.reshape(n_node, CAP, width), "node", split_axis=0, concat_axis=0, tiled=True
    ).reshape(rows_dev, width)
    rows = lax.all_gather(arrived, "local", axis=0, tiled=True)
    gate_proj = jnp.dot(rows, w_gate[0], preferred_element_type=jnp.float32)
    up_proj = jnp.dot(rows, w_up[0], preferred_element_type=jnp.float32)
    hidden = (jax.nn.silu(gate_proj) * up_proj).astype(jnp.bfloat16)
    parts = jnp.dot(hidden, w_down[0], preferred_element_type=jnp.float32).astype(jnp.bfloat16)
    expert_out = lax.psum_scatter(parts, "local", scatter_dimension=0, tiled=True)
    returned = lax.all_to_all(
        expert_out.reshape(n_node, CAP, width), "node", split_axis=0, concat_axis=0, tiled=True
    ).reshape(rows_dev, width)
    handed = passed_along(returned, "section", 1)
    combined = jnp.einsum(
        "ct,cd->td", weights, handed.astype(jnp.float32), precision=lax.Precision.HIGHEST
    )
    return combined.astype(jnp.bfloat16)[None]


def solution(mesh):
    placed = (
        P("section", ("node", "local"), None),
        P("section", ("node", "local"), None),
        P("section", ("node", "local"), None),
        P(),
        P("node", None, "local"),
        P("node", None, "local"),
        P("node", "local", None),
    )
    return jax.shard_map(
        shards,
        mesh=mesh,
        in_specs=placed,
        out_specs=P("section", ("node", "local"), None),
        check_vma=False,
    )
```

```python
import jax
import jax.numpy as jnp
from jax import lax
from jax.experimental import pallas as pl
from jax.experimental.pallas import tpu as pltpu
from jax.sharding import PartitionSpec as P

CAP = 2
COLUMNS = 896
VMEM = pl.BlockSpec(memory_space=pltpu.VMEM)
ANY = pl.BlockSpec(memory_space=pl.ANY)


def grant(mib):
    return pltpu.CompilerParams(vmem_limit_bytes=mib * 1024 * 1024)


def cost(flops, moved):
    return pl.CostEstimate(flops=flops, bytes_accessed=moved, transcendentals=0)


def pick_kernel(table_ref, routes_ref, gates_ref, tokens_ref, rows_ref, combine_ref):
    slots = table_ref.shape[0]
    rows_dev = rows_ref.shape[0]
    tok_dev = tokens_ref.shape[0]
    picks = routes_ref[...]
    gates = gates_ref[...]
    row_slot = lax.broadcasted_iota(jnp.int32, (rows_dev, tok_dev), 0) // CAP
    row_pos = lax.broadcasted_iota(jnp.int32, (rows_dev, tok_dev), 0) % CAP
    named = jnp.zeros((rows_dev, tok_dev), jnp.float32)
    weight = jnp.zeros((rows_dev, tok_dev), jnp.float32)
    want = jnp.zeros((rows_dev, tok_dev), jnp.int32)
    for s in range(slots):
        expert = table_ref[s]
        copies = jnp.int32(0)
        earlier = jnp.int32(0)
        for other in range(slots):
            same = (table_ref[other] == expert).astype(jnp.int32)
            copies = copies + same
            if other < s:
                earlier = earlier + same
        match = picks == expert
        named_s = jnp.sum(match.astype(jnp.float32), axis=0, keepdims=True)
        weight_s = jnp.sum(jnp.where(match, gates, 0.0), axis=0, keepdims=True)
        here = row_slot == s
        named = jnp.where(here, named_s, named)
        weight = jnp.where(here, weight_s, weight)
        want = jnp.where(here, row_pos * copies + earlier, want)
    before = lax.broadcasted_iota(jnp.int32, (tok_dev, tok_dev), 0)
    after = lax.broadcasted_iota(jnp.int32, (tok_dev, tok_dev), 1)
    triangle = (before < after).astype(jnp.float32).astype(jnp.bfloat16)
    rank = jnp.dot(named.astype(jnp.bfloat16), triangle, preferred_element_type=jnp.float32)
    chosen = (named > 0.0) & (rank == want.astype(jnp.float32))
    combine_ref[...] = jnp.where(chosen, weight, 0.0)
    select = jnp.where(chosen, 1.0, 0.0).astype(jnp.bfloat16)
    rows_ref[...] = jnp.dot(select, tokens_ref[...], preferred_element_type=jnp.float32).astype(
        jnp.bfloat16
    )


def pick_rows(table, picks, gates, tokens, rows_dev):
    tok_dev, width = tokens.shape
    return pl.pallas_call(
        pick_kernel,
        out_shape=(
            jax.ShapeDtypeStruct((rows_dev, width), jnp.bfloat16),
            jax.ShapeDtypeStruct((rows_dev, tok_dev), jnp.float32),
        ),
        in_specs=[pl.BlockSpec(memory_space=pltpu.SMEM), VMEM, VMEM, VMEM],
        out_specs=(VMEM, VMEM),
        compiler_params=grant(8),
        cost_estimate=cost(2 * rows_dev * tok_dev * width, 2 * (tok_dev + rows_dev) * width),
        name="pick_rows",
    )(table, picks, gates, tokens)


def experts_kernel(n, *refs):
    blocks, (gate_ref, up_ref, down_ref), outs = refs[:n], refs[n : n + 3], refs[n + 4 :]
    rows_dev, width = blocks[0].shape
    hid = gate_ref.shape[1]
    gate_proj = jnp.zeros((n * rows_dev, hid), jnp.float32)
    up_proj = jnp.zeros((n * rows_dev, hid), jnp.float32)
    for c in range(0, width, COLUMNS):
        cols = slice(c, min(c + COLUMNS, width))
        rows = jnp.concatenate([b[:, cols] for b in blocks], axis=0)
        gate_proj += jnp.dot(rows, gate_ref[cols, :], preferred_element_type=jnp.float32)
        up_proj += jnp.dot(rows, up_ref[cols, :], preferred_element_type=jnp.float32)
    silu = gate_proj / (1.0 + jnp.exp(-gate_proj))
    hidden = (silu * up_proj).astype(jnp.bfloat16)
    for c in range(0, width, COLUMNS):
        cols = slice(c, min(c + COLUMNS, width))
        part = jnp.dot(hidden, down_ref[:, cols], preferred_element_type=jnp.float32)
        part = part.astype(jnp.bfloat16)
        for k in range(n):
            outs[k][:, cols] = part[k * rows_dev : (k + 1) * rows_dev]


def experts(blocks, w_gate, w_up, w_down, after):
    n = len(blocks)
    rows_dev, width = blocks[0].shape
    hid = w_gate.shape[1]
    return pl.pallas_call(
        lambda *refs: experts_kernel(n, *refs),
        out_shape=[jax.ShapeDtypeStruct((rows_dev, width), jnp.bfloat16)] * n,
        in_specs=[VMEM] * (n + 3) + [ANY],
        out_specs=[VMEM] * n,
        compiler_params=grant(24),
        cost_estimate=cost(6 * n * rows_dev * width * hid, 6 * width * hid),
        name="experts",
    )(*blocks, w_gate, w_up, w_down, after)


def plus_kernel(*refs):
    total = refs[0][...].astype(jnp.float32)
    for ref in refs[1:-1]:
        total = total + ref[...].astype(jnp.float32)
    refs[-1][...] = total.astype(jnp.bfloat16)


def plus(*terms, after=None):
    held = () if after is None else (after,)
    body = plus_kernel if after is None else (lambda *r: plus_kernel(*r[:-2], r[-1]))
    return pl.pallas_call(
        body,
        out_shape=jax.ShapeDtypeStruct(terms[0].shape, jnp.bfloat16),
        in_specs=[VMEM] * len(terms) + [ANY] * len(held),
        out_specs=VMEM,
        compiler_params=grant(4),
        cost_estimate=cost(len(terms) * terms[0].size, 2 * (len(terms) + 1) * terms[0].size),
        name="plus",
    )(*terms, *held)


def combine_kernel(weights_ref, rows_ref, out_ref):
    weights = weights_ref[...]
    high = weights.astype(jnp.bfloat16)
    rest = weights - high.astype(jnp.float32)
    middle = rest.astype(jnp.bfloat16)
    low = (rest - middle.astype(jnp.float32)).astype(jnp.bfloat16)
    split = jnp.concatenate([high, middle, low], axis=0)
    rows = rows_ref[...]
    rows = jnp.concatenate([rows, rows, rows], axis=0)
    out_ref[...] = lax.dot_general(
        split, rows, (((0,), (0,)), ((), ())), preferred_element_type=jnp.float32
    ).astype(jnp.bfloat16)


def combine_rows(weights, rows):
    rows_dev, tok_dev = weights.shape
    width = rows.shape[1]
    block = width // 4
    return pl.pallas_call(
        combine_kernel,
        grid=(4,),
        out_shape=jax.ShapeDtypeStruct((tok_dev, width), jnp.bfloat16),
        in_specs=[
            pl.BlockSpec((rows_dev, tok_dev), lambda j: (0, 0)),
            pl.BlockSpec((rows_dev, block), lambda j: (0, j)),
        ],
        out_specs=pl.BlockSpec((tok_dev, block), lambda j: (0, j)),
        compiler_params=grant(8),
        cost_estimate=cost(6 * rows_dev * tok_dev * width, 2 * (tok_dev + rows_dev) * width),
        name="combine_rows",
    )(weights, rows)


def hop(block, step, sections=0):
    count = lax.axis_size("section")
    nodes = lax.axis_size("node")
    n = lax.axis_size("local")
    pairs = []
    for s in range(count - sections):
        for node in range(nodes):
            way = step if node % 2 == 0 else -step
            for i in range(n):
                source = (s * nodes + node) * n + i
                pairs.append((source, ((s + sections) * nodes + node) * n + (i + way) % n))
    return lax.ppermute(block, ("section", "node", "local"), pairs)


def shards(tokens, routes, route_gates, replica_table, w_gate, w_up, w_down):
    n_node = lax.axis_size("node")
    far = lax.axis_size("local") // 2
    rows_dev = n_node * CAP
    width = tokens.shape[2]
    outgoing, combine = pick_rows(replica_table, routes[0].T, route_gates[0].T, tokens[0], rows_dev)
    weights = hop(combine, 0, 1)
    own = lax.all_to_all(
        outgoing.reshape(n_node, CAP, width), "node", split_axis=0, concat_axis=0, tiled=True
    ).reshape(rows_dev, width)
    blocks = {0: own}
    ahead, back = own, own
    for q in range(1, far):
        ahead, back = hop(ahead, 1), hop(back, -1)
        blocks[-q], blocks[q] = ahead, back
    blocks[far] = hop(ahead, 1)
    order = sorted(blocks)
    parts = experts([blocks[q] for q in order], w_gate[0], w_up[0], w_down[0], weights)
    part = dict(zip(order, parts))
    mine = hop(part[0], 0, 1)
    ahead, back = hop(part[far], 1), hop(part[1 - far], -1)
    for q in range(far - 1, 0, -1):
        last = q == 1
        ahead = plus(part[q], ahead, after=mine if last else None)
        if not last:
            back = hop(plus(part[1 - q], back), -1, 1 if q == 2 else 0)
        ahead = hop(ahead, 1, 1 if last else 0)
    expert_out = plus(mine, back, ahead)
    returned = lax.all_to_all(
        expert_out.reshape(n_node, CAP, width), "node", split_axis=0, concat_axis=0, tiled=True
    ).reshape(rows_dev, width)
    return combine_rows(weights, returned)[None]


def solution(mesh):
    placed = (
        P("section", ("node", "local"), None),
        P("section", ("node", "local"), None),
        P("section", ("node", "local"), None),
        P(),
        P("node", None, "local"),
        P("node", None, "local"),
        P("node", "local", None),
    )
    return jax.shard_map(
        shards,
        mesh=mesh,
        in_specs=placed,
        out_specs=P("section", ("node", "local"), None),
        check_vma=False,
    )
```

```python
import jax
import jax.numpy as jnp
from jax import lax
from jax.experimental import pallas as pl
from jax.experimental.pallas import tpu as pltpu
from jax.sharding import PartitionSpec as P

CAP = 2
COLUMNS = 896
PIECE = 1792
VMEM = pl.BlockSpec(memory_space=pltpu.VMEM)
ANY = pl.BlockSpec(memory_space=pl.ANY)
HBM = pl.BlockSpec(memory_space=pltpu.HBM)


def grant(mib):
    return pltpu.CompilerParams(vmem_limit_bytes=mib * 1024 * 1024)


def cost(flops, moved):
    return pl.CostEstimate(flops=flops, bytes_accessed=moved, transcendentals=0)


def pick_kernel(
    table_ref, routes_hbm, gates_hbm, tokens_hbm, rows_ref, combine_ref, routes_ref, gates_ref, tokens_ref, arrived
):
    slots = table_ref.shape[0]
    rows_dev = rows_ref.shape[0]
    tok_dev, width = tokens_ref.shape
    starts = range(0, width, PIECE)
    small = [
        pltpu.make_async_copy(routes_hbm, routes_ref, arrived.at[0]),
        pltpu.make_async_copy(gates_hbm, gates_ref, arrived.at[1]),
    ]
    pieces = []
    for k, c in enumerate(starts):
        cols = pl.ds(c, min(PIECE, width - c))
        pieces.append(
            pltpu.make_async_copy(tokens_hbm.at[:, cols], tokens_ref.at[:, cols], arrived.at[2 + k])
        )
    for copy in small + pieces:
        copy.start()
    for copy in small:
        copy.wait()
    picks = routes_ref[...]
    gates = gates_ref[...]
    row_slot = lax.broadcasted_iota(jnp.int32, (rows_dev, tok_dev), 0) // CAP
    row_pos = lax.broadcasted_iota(jnp.int32, (rows_dev, tok_dev), 0) % CAP
    named = jnp.zeros((rows_dev, tok_dev), jnp.float32)
    weight = jnp.zeros((rows_dev, tok_dev), jnp.float32)
    want = jnp.zeros((rows_dev, tok_dev), jnp.int32)
    for s in range(slots):
        expert = table_ref[s]
        copies = jnp.int32(0)
        earlier = jnp.int32(0)
        for other in range(slots):
            same = (table_ref[other] == expert).astype(jnp.int32)
            copies = copies + same
            if other < s:
                earlier = earlier + same
        match = picks == expert
        named_s = jnp.sum(match.astype(jnp.float32), axis=0, keepdims=True)
        weight_s = jnp.sum(jnp.where(match, gates, 0.0), axis=0, keepdims=True)
        here = row_slot == s
        named = jnp.where(here, named_s, named)
        weight = jnp.where(here, weight_s, weight)
        want = jnp.where(here, row_pos * copies + earlier, want)
    before = lax.broadcasted_iota(jnp.int32, (tok_dev, tok_dev), 0)
    after = lax.broadcasted_iota(jnp.int32, (tok_dev, tok_dev), 1)
    triangle = (before < after).astype(jnp.float32).astype(jnp.bfloat16)
    rank = jnp.dot(named.astype(jnp.bfloat16), triangle, preferred_element_type=jnp.float32)
    chosen = (named > 0.0) & (rank == want.astype(jnp.float32))
    combine_ref[...] = jnp.where(chosen, weight, 0.0)
    select = jnp.where(chosen, 1.0, 0.0).astype(jnp.bfloat16)
    for copy, c in zip(pieces, starts):
        copy.wait()
        cols = slice(c, min(c + PIECE, width))
        rows_ref[:, cols] = jnp.dot(
            select, tokens_ref[:, cols], preferred_element_type=jnp.float32
        ).astype(jnp.bfloat16)


def pick_rows(table, picks, gates, tokens, rows_dev):
    tok_dev, width = tokens.shape
    return pl.pallas_call(
        pick_kernel,
        out_shape=(
            jax.ShapeDtypeStruct((rows_dev, width), jnp.bfloat16),
            jax.ShapeDtypeStruct((rows_dev, tok_dev), jnp.float32),
        ),
        in_specs=[pl.BlockSpec(memory_space=pltpu.SMEM), HBM, HBM, HBM],
        out_specs=(VMEM, VMEM),
        scratch_shapes=[
            pltpu.VMEM(picks.shape, picks.dtype),
            pltpu.VMEM(gates.shape, gates.dtype),
            pltpu.VMEM(tokens.shape, tokens.dtype),
            pltpu.SemaphoreType.DMA((2 + -(-width // PIECE),)),
        ],
        cost_estimate=cost(2 * rows_dev * tok_dev * width, 2 * (tok_dev + rows_dev) * width),
        name="pick_rows",
    )(table, picks, gates, tokens)


def load_kernel(n, *refs):
    sources, targets, arrived = refs[:n], refs[n + 1 : 2 * n + 1], refs[2 * n + 1]
    copies = [
        pltpu.make_async_copy(source, target, arrived.at[k])
        for k, (source, target) in enumerate(zip(sources, targets))
    ]
    for copy in copies:
        copy.start()
    for copy in copies:
        copy.wait()


def load(arrays, after):
    n = len(arrays)
    return pl.pallas_call(
        lambda *refs: load_kernel(n, *refs),
        out_shape=[jax.ShapeDtypeStruct(a.shape, a.dtype) for a in arrays],
        in_specs=[HBM] * n + [ANY],
        out_specs=[VMEM] * n,
        scratch_shapes=[pltpu.SemaphoreType.DMA((n,))],
        compiler_params=grant(16),
        cost_estimate=cost(1_000_000_000, sum(2 * a.size * a.dtype.itemsize for a in arrays)),
        name="load",
    )(*arrays, after)


def experts_kernel(n, *refs):
    blocks, (gate_ref, up_ref, down_ref), outs = refs[:n], refs[n : n + 3], refs[n + 3 :]
    rows_dev, width = blocks[0].shape
    hid = gate_ref.shape[1]
    gate_proj = jnp.zeros((n * rows_dev, hid), jnp.float32)
    up_proj = jnp.zeros((n * rows_dev, hid), jnp.float32)
    for c in range(0, width, COLUMNS):
        cols = slice(c, min(c + COLUMNS, width))
        rows = jnp.concatenate([b[:, cols] for b in blocks], axis=0)
        gate_proj += jnp.dot(rows, gate_ref[cols, :], preferred_element_type=jnp.float32)
        up_proj += jnp.dot(rows, up_ref[cols, :], preferred_element_type=jnp.float32)
    silu = gate_proj / (1.0 + jnp.exp(-gate_proj))
    hidden = (silu * up_proj).astype(jnp.bfloat16)
    for c in range(0, width, COLUMNS):
        cols = slice(c, min(c + COLUMNS, width))
        part = jnp.dot(hidden, down_ref[:, cols], preferred_element_type=jnp.float32)
        part = part.astype(jnp.bfloat16)
        for k in range(n):
            outs[k][:, cols] = part[k * rows_dev : (k + 1) * rows_dev]


def experts(blocks, w_gate, w_up, w_down):
    n = len(blocks)
    rows_dev, width = blocks[0].shape
    hid = w_gate.shape[1]
    return pl.pallas_call(
        lambda *refs: experts_kernel(n, *refs),
        out_shape=[jax.ShapeDtypeStruct((rows_dev, width), jnp.bfloat16)] * n,
        in_specs=[VMEM] * (n + 3),
        out_specs=[VMEM] * n,
        compiler_params=grant(24),
        cost_estimate=cost(6 * n * rows_dev * width * hid, 6 * width * hid),
        name="experts",
    )(*blocks, w_gate, w_up, w_down)


def plus_kernel(*refs):
    total = refs[0][...].astype(jnp.float32)
    for ref in refs[1:-1]:
        total = total + ref[...].astype(jnp.float32)
    refs[-1][...] = total.astype(jnp.bfloat16)


def plus(*terms, after=None):
    held = () if after is None else (after,)
    body = plus_kernel if after is None else (lambda *r: plus_kernel(*r[:-2], r[-1]))
    return pl.pallas_call(
        body,
        out_shape=jax.ShapeDtypeStruct(terms[0].shape, jnp.bfloat16),
        in_specs=[VMEM] * len(terms) + [ANY] * len(held),
        out_specs=VMEM,
        compiler_params=grant(4),
        cost_estimate=cost(len(terms) * terms[0].size, 2 * (len(terms) + 1) * terms[0].size),
        name="plus",
    )(*terms, *held)


def combine_kernel(weights_ref, rows_ref, out_ref):
    weights = weights_ref[...]
    high = weights.astype(jnp.bfloat16)
    rest = weights - high.astype(jnp.float32)
    middle = rest.astype(jnp.bfloat16)
    low = (rest - middle.astype(jnp.float32)).astype(jnp.bfloat16)
    split = jnp.concatenate([high, middle, low], axis=0)
    rows = rows_ref[...]
    rows = jnp.concatenate([rows, rows, rows], axis=0)
    out_ref[...] = lax.dot_general(
        split, rows, (((0,), (0,)), ((), ())), preferred_element_type=jnp.float32
    ).astype(jnp.bfloat16)


def combine_rows(weights, rows):
    rows_dev, tok_dev = weights.shape
    width = rows.shape[1]
    block = width // 4
    return pl.pallas_call(
        combine_kernel,
        grid=(4,),
        out_shape=jax.ShapeDtypeStruct((tok_dev, width), jnp.bfloat16),
        in_specs=[
            pl.BlockSpec((rows_dev, tok_dev), lambda j: (0, 0)),
            pl.BlockSpec((rows_dev, block), lambda j: (0, j)),
        ],
        out_specs=pl.BlockSpec((tok_dev, block), lambda j: (0, j)),
        compiler_params=grant(8),
        cost_estimate=cost(6 * rows_dev * tok_dev * width, 2 * (tok_dev + rows_dev) * width),
        name="combine_rows",
    )(weights, rows)


def hop(block, step, sections=0):
    count = lax.axis_size("section")
    nodes = lax.axis_size("node")
    n = lax.axis_size("local")
    pairs = []
    for s in range(count - sections):
        for node in range(nodes):
            way = step if node % 2 == 0 else -step
            for i in range(n):
                source = (s * nodes + node) * n + i
                pairs.append((source, ((s + sections) * nodes + node) * n + (i + way) % n))
    return lax.ppermute(block, ("section", "node", "local"), pairs)


def shards(tokens, routes, route_gates, replica_table, w_gate, w_up, w_down):
    n_node = lax.axis_size("node")
    far = lax.axis_size("local") // 2
    rows_dev = n_node * CAP
    width = tokens.shape[2]
    outgoing, combine = pick_rows(replica_table, routes[0].T, route_gates[0].T, tokens[0], rows_dev)
    weights = hop(combine, 0, 1)
    own = lax.all_to_all(
        outgoing.reshape(n_node, CAP, width), "node", split_axis=0, concat_axis=0, tiled=True
    ).reshape(rows_dev, width)
    blocks = {0: own}
    for q in range(2, 0, -1):
        blocks[-q], blocks[q] = hop(own, q), hop(own, -q)
    for q in range(3, far):
        blocks[-q], blocks[q] = hop(blocks[2 - q], 2), hop(blocks[q - 2], -2)
    blocks[far] = hop(blocks[2 - far], 2)
    order = sorted(blocks)
    up_mat, down_mat = load([w_up[0], w_down[0]], weights)
    parts = experts([blocks[q] for q in order], w_gate[0], up_mat, down_mat)
    part = dict(zip(order, parts))
    mine = hop(part[0], 0, 1)
    ahead, back = hop(part[far], 1), hop(part[1 - far], -1)
    for q in range(far - 1, 0, -1):
        last = q == 1
        ahead = plus(part[q], ahead, after=mine if last else None)
        if not last:
            back = hop(plus(part[1 - q], back), -1, 1 if q == 2 else 0)
        ahead = hop(ahead, 1, 1 if last else 0)
    expert_out = plus(mine, back, ahead)
    returned = lax.all_to_all(
        expert_out.reshape(n_node, CAP, width), "node", split_axis=0, concat_axis=0, tiled=True
    ).reshape(rows_dev, width)
    return combine_rows(weights, returned)[None]


def solution(mesh):
    placed = (
        P("section", ("node", "local"), None),
        P("section", ("node", "local"), None),
        P("section", ("node", "local"), None),
        P(),
        P("node", None, "local"),
        P("node", None, "local"),
        P("node", "local", None),
    )
    return jax.shard_map(
        shards,
        mesh=mesh,
        in_specs=placed,
        out_specs=P("section", ("node", "local"), None),
        check_vma=False,
    )
```

```python
import jax
import jax.numpy as jnp
from jax import lax
from jax.experimental import pallas as pl
from jax.experimental.pallas import tpu as pltpu
from jax.sharding import PartitionSpec as P

CAP = 2
COLUMNS = 896
PIECE = 1792
LANES = 128
SPLIT = 3
VMEM = pl.BlockSpec(memory_space=pltpu.VMEM)
ANY = pl.BlockSpec(memory_space=pl.ANY)
HBM = pl.BlockSpec(memory_space=pltpu.HBM)


def grant(mib):
    return pltpu.CompilerParams(vmem_limit_bytes=mib * 1024 * 1024)


def cost(flops, moved):
    return pl.CostEstimate(flops=flops, bytes_accessed=moved, transcendentals=0)


def pick_kernel(
    table_ref, routes_hbm, gates_hbm, tokens_hbm, rows_ref, combine_ref, routes_ref, gates_ref, tokens_ref, arrived
):
    slots = table_ref.shape[0]
    rows_dev = rows_ref.shape[0]
    tok_dev, width = tokens_ref.shape
    starts = range(0, width, PIECE)
    small = [
        pltpu.make_async_copy(routes_hbm, routes_ref, arrived.at[0]),
        pltpu.make_async_copy(gates_hbm, gates_ref, arrived.at[1]),
    ]
    pieces = []
    for k, c in enumerate(starts):
        cols = pl.ds(c, min(PIECE, width - c))
        pieces.append(
            pltpu.make_async_copy(tokens_hbm.at[:, cols], tokens_ref.at[:, cols], arrived.at[2 + k])
        )
    for copy in small + pieces:
        copy.start()
    for copy in small:
        copy.wait()
    picks = routes_ref[...]
    gates = gates_ref[...]
    row_slot = lax.broadcasted_iota(jnp.int32, (rows_dev, tok_dev), 0) // CAP
    row_pos = lax.broadcasted_iota(jnp.int32, (rows_dev, tok_dev), 0) % CAP
    named = jnp.zeros((rows_dev, tok_dev), jnp.float32)
    weight = jnp.zeros((rows_dev, tok_dev), jnp.float32)
    want = jnp.zeros((rows_dev, tok_dev), jnp.int32)
    for s in range(slots):
        expert = table_ref[s]
        copies = jnp.int32(0)
        earlier = jnp.int32(0)
        for other in range(slots):
            same = (table_ref[other] == expert).astype(jnp.int32)
            copies = copies + same
            if other < s:
                earlier = earlier + same
        match = picks == expert
        named_s = jnp.sum(match.astype(jnp.float32), axis=0, keepdims=True)
        weight_s = jnp.sum(jnp.where(match, gates, 0.0), axis=0, keepdims=True)
        here = row_slot == s
        named = jnp.where(here, named_s, named)
        weight = jnp.where(here, weight_s, weight)
        want = jnp.where(here, row_pos * copies + earlier, want)
    before = lax.broadcasted_iota(jnp.int32, (tok_dev, tok_dev), 0)
    after = lax.broadcasted_iota(jnp.int32, (tok_dev, tok_dev), 1)
    triangle = (before < after).astype(jnp.float32).astype(jnp.bfloat16)
    rank = jnp.dot(named.astype(jnp.bfloat16), triangle, preferred_element_type=jnp.float32)
    chosen = (named > 0.0) & (rank == want.astype(jnp.float32))
    weight = jnp.where(chosen, weight, 0.0)
    combine_ref[...] = jnp.zeros_like(combine_ref)
    for k in range(SPLIT):
        piece = weight.astype(jnp.bfloat16)
        weight = weight - piece.astype(jnp.float32)
        combine_ref[:, k * LANES : k * LANES + tok_dev] = piece
    select = jnp.where(chosen, 1.0, 0.0).astype(jnp.bfloat16)
    for copy, c in zip(pieces, starts):
        copy.wait()
        cols = slice(c, min(c + PIECE, width))
        rows_ref[:, cols] = jnp.dot(
            select, tokens_ref[:, cols], preferred_element_type=jnp.float32
        ).astype(jnp.bfloat16)


def pick_rows(table, picks, gates, tokens, rows_dev):
    tok_dev, width = tokens.shape
    return pl.pallas_call(
        pick_kernel,
        out_shape=(
            jax.ShapeDtypeStruct((rows_dev, width), jnp.bfloat16),
            jax.ShapeDtypeStruct((rows_dev, SPLIT * LANES), jnp.bfloat16),
        ),
        in_specs=[pl.BlockSpec(memory_space=pltpu.SMEM), HBM, HBM, HBM],
        out_specs=(VMEM, VMEM),
        scratch_shapes=[
            pltpu.VMEM(picks.shape, picks.dtype),
            pltpu.VMEM(gates.shape, gates.dtype),
            pltpu.VMEM(tokens.shape, tokens.dtype),
            pltpu.SemaphoreType.DMA((2 + -(-width // PIECE),)),
        ],
        cost_estimate=cost(2 * rows_dev * tok_dev * width, 2 * (tok_dev + rows_dev) * width),
        name="pick_rows",
    )(table, picks, gates, tokens)


def load_kernel(n, *refs):
    sources, targets, arrived = refs[:n], refs[n + 1 : 2 * n + 1], refs[2 * n + 1]
    copies = [
        pltpu.make_async_copy(source, target, arrived.at[k])
        for k, (source, target) in enumerate(zip(sources, targets))
    ]
    for copy in copies:
        copy.start()
    for copy in copies:
        copy.wait()


def load(arrays, after):
    n = len(arrays)
    return pl.pallas_call(
        lambda *refs: load_kernel(n, *refs),
        out_shape=[jax.ShapeDtypeStruct(a.shape, a.dtype) for a in arrays],
        in_specs=[HBM] * n + [ANY],
        out_specs=[VMEM] * n,
        scratch_shapes=[pltpu.SemaphoreType.DMA((n,))],
        compiler_params=grant(16),
        cost_estimate=cost(1_000_000_000, sum(2 * a.size * a.dtype.itemsize for a in arrays)),
        name="load",
    )(*arrays, after)


def experts_kernel(n, own, *refs):
    blocks, (gate_ref, up_ref, down_ref, tail_ref), outs = refs[:n], refs[n : n + 4], refs[n + 4 :]
    rows_dev, width = blocks[0].shape
    hid = gate_ref.shape[1]
    gate_proj = jnp.zeros((n * rows_dev, hid), jnp.float32)
    up_proj = jnp.zeros((n * rows_dev, hid), jnp.float32)
    for c in range(0, width, COLUMNS):
        cols = slice(c, min(c + COLUMNS, width))
        rows = jnp.concatenate([b[:, cols] for b in blocks], axis=0)
        gate_proj += jnp.dot(rows, gate_ref[cols, :], preferred_element_type=jnp.float32)
        up_proj += jnp.dot(rows, up_ref[cols, :], preferred_element_type=jnp.float32)
    silu = gate_proj / (1.0 + jnp.exp(-gate_proj))
    hidden = (silu * up_proj).astype(jnp.bfloat16)
    for c in range(0, width, COLUMNS):
        cols = slice(c, min(c + COLUMNS, width))
        part = jnp.dot(hidden, down_ref[:, cols], preferred_element_type=jnp.float32)
        part = part.astype(jnp.bfloat16)
        for k in range(n):
            outs[k][:, cols] = part[k * rows_dev : (k + 1) * rows_dev]
    outs[own][:, width:] = tail_ref[...]


def experts(blocks, w_gate, w_up, w_down, tail, own):
    n = len(blocks)
    rows_dev, width = blocks[0].shape
    hid = w_gate.shape[1]
    widths = [width + (tail.shape[1] if k == own else 0) for k in range(n)]
    return pl.pallas_call(
        lambda *refs: experts_kernel(n, own, *refs),
        out_shape=[jax.ShapeDtypeStruct((rows_dev, w), jnp.bfloat16) for w in widths],
        in_specs=[VMEM] * (n + 4),
        out_specs=[VMEM] * n,
        compiler_params=grant(24),
        cost_estimate=cost(6 * n * rows_dev * width * hid, 6 * width * hid),
        name="experts",
    )(*blocks, w_gate, w_up, w_down, tail)


def plus_kernel(*refs):
    out_ref = refs[-1]
    width = out_ref.shape[1]
    total = refs[0][:, :width].astype(jnp.float32)
    for ref in refs[1:-1]:
        total = total + ref[:, :width].astype(jnp.float32)
    out_ref[...] = total.astype(jnp.bfloat16)


def plus(*terms):
    shape = terms[-1].shape
    size = shape[0] * shape[1]
    return pl.pallas_call(
        plus_kernel,
        out_shape=jax.ShapeDtypeStruct(shape, jnp.bfloat16),
        in_specs=[VMEM] * len(terms),
        out_specs=VMEM,
        compiler_params=grant(4),
        cost_estimate=cost(len(terms) * size, 2 * (len(terms) + 1) * size),
        name="plus",
    )(*terms)


def combine_kernel(*refs):
    pieces, rows_ref, out_ref = refs[:SPLIT], refs[SPLIT], refs[SPLIT + 1]
    tok_dev = out_ref.shape[0]
    split = jnp.concatenate([piece[...] for piece in pieces], axis=0)
    rows = rows_ref[...]
    rows = jnp.concatenate([rows] * SPLIT, axis=0)
    out = lax.dot_general(split, rows, (((0,), (0,)), ((), ())), preferred_element_type=jnp.float32)
    out_ref[...] = out[:tok_dev].astype(jnp.bfloat16)


def combine_rows(carrier, rows, tok_dev):
    rows_dev, width = rows.shape
    block = width // 4
    tail = [
        pl.BlockSpec((rows_dev, LANES), lambda j, k=k: (0, width // LANES + k)) for k in range(SPLIT)
    ]
    return pl.pallas_call(
        combine_kernel,
        grid=(4,),
        out_shape=jax.ShapeDtypeStruct((tok_dev, width), jnp.bfloat16),
        in_specs=tail + [pl.BlockSpec((rows_dev, block), lambda j: (0, j))],
        out_specs=pl.BlockSpec((tok_dev, block), lambda j: (0, j)),
        compiler_params=grant(8),
        cost_estimate=cost(6 * rows_dev * tok_dev * width, 2 * (tok_dev + rows_dev) * width),
        name="combine_rows",
    )(*([carrier] * SPLIT), rows)


def hop(block, step, sections=0):
    count = lax.axis_size("section")
    nodes = lax.axis_size("node")
    n = lax.axis_size("local")
    pairs = []
    for s in range(count - sections):
        for node in range(nodes):
            way = step if node % 2 == 0 else -step
            for i in range(n):
                source = (s * nodes + node) * n + i
                pairs.append((source, ((s + sections) * nodes + node) * n + (i + way) % n))
    return lax.ppermute(block, ("section", "node", "local"), pairs)


def shards(tokens, routes, route_gates, replica_table, w_gate, w_up, w_down):
    n_node = lax.axis_size("node")
    far = lax.axis_size("local") // 2
    rows_dev = n_node * CAP
    width = tokens.shape[2]
    outgoing, tail = pick_rows(replica_table, routes[0].T, route_gates[0].T, tokens[0], rows_dev)
    own = lax.all_to_all(
        outgoing.reshape(n_node, CAP, width), "node", split_axis=0, concat_axis=0, tiled=True
    ).reshape(rows_dev, width)
    blocks = {0: own}
    blocks[-2], blocks[2] = hop(own, 2), hop(own, -2)
    blocks[-1], blocks[1] = hop(own, 1), hop(own, -1)
    blocks[far] = hop(blocks[-2], 2)
    blocks[-3], blocks[3] = hop(blocks[-2], 1), hop(blocks[2], -1)
    order = sorted(blocks)
    up_mat, down_mat = load([w_up[0], w_down[0]], blocks[-1])
    parts = experts(
        [blocks[q] for q in order], w_gate[0], up_mat, down_mat, tail, order.index(0)
    )
    part = dict(zip(order, parts))
    ahead = plus(part[2], hop(part[far], 2), hop(part[3], 1))
    back = plus(part[-2], hop(part[-3], -1))
    carrier = hop(part[0], 0, 1)
    near = [hop(part[1], 1, 1), hop(part[-1], -1, 1)]
    expert_out = plus(carrier, *near, hop(ahead, 2, 1), hop(back, -2, 1))
    returned = lax.all_to_all(
        expert_out.reshape(n_node, CAP, width), "node", split_axis=0, concat_axis=0, tiled=True
    ).reshape(rows_dev, width)
    return combine_rows(carrier, returned, tokens.shape[1])[None]


def solution(mesh):
    placed = (
        P("section", ("node", "local"), None),
        P("section", ("node", "local"), None),
        P("section", ("node", "local"), None),
        P(),
        P("node", None, "local"),
        P("node", None, "local"),
        P("node", "local", None),
    )
    return jax.shard_map(
        shards,
        mesh=mesh,
        in_specs=placed,
        out_specs=P("section", ("node", "local"), None),
        check_vma=False,
    )
```

```python
import jax
import jax.numpy as jnp
from jax import lax
from jax.experimental import pallas as pl
from jax.experimental.pallas import tpu as pltpu
from jax.sharding import PartitionSpec as P

CAP = 2
COLUMNS = 896
PIECE = 1792
LANES = 128
SPLIT = 3
VMEM = pl.BlockSpec(memory_space=pltpu.VMEM)
ANY = pl.BlockSpec(memory_space=pl.ANY)
HBM = pl.BlockSpec(memory_space=pltpu.HBM)


def grant(mib):
    return pltpu.CompilerParams(vmem_limit_bytes=mib * 1024 * 1024)


def cost(flops, moved):
    return pl.CostEstimate(flops=flops, bytes_accessed=moved, transcendentals=0)


def pick_kernel(
    table_ref, routes_hbm, gates_hbm, tokens_hbm, rows_ref, combine_ref, routes_ref, gates_ref, tokens_ref, arrived
):
    slots = table_ref.shape[0]
    rows_dev = combine_ref.shape[0]
    tok_dev, width = tokens_ref.shape
    starts = range(0, width, PIECE)
    small = [
        pltpu.make_async_copy(routes_hbm, routes_ref, arrived.at[0]),
        pltpu.make_async_copy(gates_hbm, gates_ref, arrived.at[1]),
    ]
    pieces = []
    for k, c in enumerate(starts):
        cols = pl.ds(c, min(PIECE, width - c))
        pieces.append(
            pltpu.make_async_copy(tokens_hbm.at[:, cols], tokens_ref.at[:, cols], arrived.at[2 + k])
        )
    for copy in small + pieces:
        copy.start()
    for copy in small:
        copy.wait()
    picks = routes_ref[...]
    gates = gates_ref[...]
    row_slot = lax.broadcasted_iota(jnp.int32, (rows_dev, tok_dev), 0) // CAP
    row_pos = lax.broadcasted_iota(jnp.int32, (rows_dev, tok_dev), 0) % CAP
    named = jnp.zeros((rows_dev, tok_dev), jnp.float32)
    weight = jnp.zeros((rows_dev, tok_dev), jnp.float32)
    want = jnp.zeros((rows_dev, tok_dev), jnp.int32)
    for s in range(slots):
        expert = table_ref[s]
        copies = jnp.int32(0)
        earlier = jnp.int32(0)
        for other in range(slots):
            same = (table_ref[other] == expert).astype(jnp.int32)
            copies = copies + same
            if other < s:
                earlier = earlier + same
        match = picks == expert
        named_s = jnp.sum(match.astype(jnp.float32), axis=0, keepdims=True)
        weight_s = jnp.sum(jnp.where(match, gates, 0.0), axis=0, keepdims=True)
        here = row_slot == s
        named = jnp.where(here, named_s, named)
        weight = jnp.where(here, weight_s, weight)
        want = jnp.where(here, row_pos * copies + earlier, want)
    before = lax.broadcasted_iota(jnp.int32, (tok_dev, tok_dev), 0)
    after = lax.broadcasted_iota(jnp.int32, (tok_dev, tok_dev), 1)
    triangle = (before < after).astype(jnp.float32).astype(jnp.bfloat16)
    rank = jnp.dot(named.astype(jnp.bfloat16), triangle, preferred_element_type=jnp.float32)
    chosen = (named > 0.0) & (rank == want.astype(jnp.float32))
    weight = jnp.where(chosen, weight, 0.0)
    combine_ref[...] = jnp.zeros_like(combine_ref)
    for k in range(SPLIT):
        piece = weight.astype(jnp.bfloat16)
        weight = weight - piece.astype(jnp.float32)
        combine_ref[:, k * LANES : k * LANES + tok_dev] = piece
    select = jnp.where(chosen, 1.0, 0.0).astype(jnp.bfloat16)
    for copy, c in zip(pieces, starts):
        copy.wait()
        cols = slice(c, min(c + PIECE, width))
        rows = jnp.dot(select, tokens_ref[:, cols], preferred_element_type=jnp.float32)
        rows_ref[:, :, cols] = rows.reshape(slots, CAP, rows.shape[1]).astype(jnp.bfloat16)


def pick_rows(table, picks, gates, tokens, rows_dev):
    tok_dev, width = tokens.shape
    return pl.pallas_call(
        pick_kernel,
        out_shape=(
            jax.ShapeDtypeStruct((rows_dev // CAP, CAP, width), jnp.bfloat16),
            jax.ShapeDtypeStruct((rows_dev, SPLIT * LANES), jnp.bfloat16),
        ),
        in_specs=[pl.BlockSpec(memory_space=pltpu.SMEM), HBM, HBM, HBM],
        out_specs=(VMEM, VMEM),
        scratch_shapes=[
            pltpu.VMEM(picks.shape, picks.dtype),
            pltpu.VMEM(gates.shape, gates.dtype),
            pltpu.VMEM(tokens.shape, tokens.dtype),
            pltpu.SemaphoreType.DMA((2 + -(-width // PIECE),)),
        ],
        cost_estimate=cost(2 * rows_dev * tok_dev * width, 2 * (tok_dev + rows_dev) * width),
        name="pick_rows",
    )(table, picks, gates, tokens)


def load_kernel(n, *refs):
    sources, targets, arrived = refs[:n], refs[n + 1 : 2 * n + 1], refs[2 * n + 1]
    copies = [
        pltpu.make_async_copy(source, target, arrived.at[k])
        for k, (source, target) in enumerate(zip(sources, targets))
    ]
    for copy in copies:
        copy.start()
    for copy in copies:
        copy.wait()


def load(arrays, after):
    n = len(arrays)
    return pl.pallas_call(
        lambda *refs: load_kernel(n, *refs),
        out_shape=[jax.ShapeDtypeStruct(a.shape, a.dtype) for a in arrays],
        in_specs=[HBM] * n + [ANY],
        out_specs=[VMEM] * n,
        scratch_shapes=[pltpu.SemaphoreType.DMA((n,))],
        compiler_params=grant(16),
        cost_estimate=cost(1_000_000_000, sum(2 * a.size * a.dtype.itemsize for a in arrays)),
        name="load",
    )(*arrays, after)


def experts_kernel(n, own, *refs):
    blocks, (gate_ref, up_ref, down_ref, tail_ref), outs = refs[:n], refs[n : n + 4], refs[n + 4 :]
    rows_dev, width = blocks[0].shape
    hid = gate_ref.shape[1]
    gate_proj = jnp.zeros((n * rows_dev, hid), jnp.float32)
    up_proj = jnp.zeros((n * rows_dev, hid), jnp.float32)
    for c in range(0, width, COLUMNS):
        cols = slice(c, min(c + COLUMNS, width))
        rows = jnp.concatenate([b[:, cols] for b in blocks], axis=0)
        gate_proj += jnp.dot(rows, gate_ref[cols, :], preferred_element_type=jnp.float32)
        up_proj += jnp.dot(rows, up_ref[cols, :], preferred_element_type=jnp.float32)
    silu = gate_proj / (1.0 + jnp.exp(-gate_proj))
    hidden = (silu * up_proj).astype(jnp.bfloat16)
    for c in range(0, width, COLUMNS):
        cols = slice(c, min(c + COLUMNS, width))
        part = jnp.dot(hidden, down_ref[:, cols], preferred_element_type=jnp.float32)
        part = part.astype(jnp.bfloat16)
        for k in range(n):
            outs[k][:, cols] = part[k * rows_dev : (k + 1) * rows_dev]
    outs[own][:, width:] = tail_ref[...]


def experts(blocks, w_gate, w_up, w_down, tail, own):
    n = len(blocks)
    rows_dev, width = blocks[0].shape
    hid = w_gate.shape[1]
    widths = [width + (tail.shape[1] if k == own else 0) for k in range(n)]
    return pl.pallas_call(
        lambda *refs: experts_kernel(n, own, *refs),
        out_shape=[jax.ShapeDtypeStruct((rows_dev, w), jnp.bfloat16) for w in widths],
        in_specs=[VMEM] * (n + 4),
        out_specs=[VMEM] * n,
        compiler_params=grant(24),
        cost_estimate=cost(6 * n * rows_dev * width * hid, 6 * width * hid),
        name="experts",
    )(*blocks, w_gate, w_up, w_down, tail)


def plus_kernel(*refs):
    out_ref = refs[-1]
    width = min(ref.shape[1] for ref in refs)
    total = refs[0][:, :width].astype(jnp.float32)
    for ref in refs[1:-1]:
        total = total + ref[:, :width].astype(jnp.float32)
    out_ref[:, :width] = total.astype(jnp.bfloat16)
    if out_ref.shape[1] > width:
        out_ref[:, width:] = refs[0][:, width:]


def plus(*terms, width=None):
    shape = (terms[0].shape[0], width or terms[0].shape[1])
    size = shape[0] * shape[1]
    return pl.pallas_call(
        plus_kernel,
        out_shape=jax.ShapeDtypeStruct(shape, jnp.bfloat16),
        in_specs=[VMEM] * len(terms),
        out_specs=VMEM,
        compiler_params=grant(4),
        cost_estimate=cost(len(terms) * size, 2 * (len(terms) + 1) * size),
        name="plus",
    )(*terms)


def combine_kernel(*refs):
    pieces, rows_ref, out_ref = refs[:SPLIT], refs[SPLIT], refs[SPLIT + 1]
    tok_dev = out_ref.shape[0]
    split = jnp.concatenate([piece[...] for piece in pieces], axis=0)
    rows = rows_ref[...]
    rows = jnp.concatenate([rows] * SPLIT, axis=0)
    out = lax.dot_general(split, rows, (((0,), (0,)), ((), ())), preferred_element_type=jnp.float32)
    out_ref[...] = out[:tok_dev].astype(jnp.bfloat16)


def combine_rows(carrier, rows, tok_dev):
    rows_dev, width = rows.shape
    block = width // 4
    tail = [
        pl.BlockSpec((rows_dev, LANES), lambda j, k=k: (0, width // LANES + k)) for k in range(SPLIT)
    ]
    return pl.pallas_call(
        combine_kernel,
        grid=(4,),
        out_shape=jax.ShapeDtypeStruct((tok_dev, width), jnp.bfloat16),
        in_specs=tail + [pl.BlockSpec((rows_dev, block), lambda j: (0, j))],
        out_specs=pl.BlockSpec((tok_dev, block), lambda j: (0, j)),
        compiler_params=grant(8),
        cost_estimate=cost(6 * rows_dev * tok_dev * width, 2 * (tok_dev + rows_dev) * width),
        name="combine_rows",
    )(*([carrier] * SPLIT), rows)


def hop(block, step, sections=0):
    count = lax.axis_size("section")
    nodes = lax.axis_size("node")
    n = lax.axis_size("local")
    pairs = []
    for s in range(count - sections):
        for node in range(nodes):
            way = step if node % 2 == 0 else -step
            for i in range(n):
                source = (s * nodes + node) * n + i
                pairs.append((source, ((s + sections) * nodes + node) * n + (i + way) % n))
    return lax.ppermute(block, ("section", "node", "local"), pairs)


def shards(tokens, routes, route_gates, replica_table, w_gate, w_up, w_down):
    n_node = lax.axis_size("node")
    far = lax.axis_size("local") // 2
    rows_dev = n_node * CAP
    width = tokens.shape[2]
    outgoing, tail = pick_rows(replica_table, routes[0].T, route_gates[0].T, tokens[0], rows_dev)
    own = lax.all_to_all(outgoing, "node", split_axis=0, concat_axis=0, tiled=True).reshape(
        rows_dev, width
    )
    blocks = {0: own}
    blocks[-2], blocks[2] = hop(own, 2), hop(own, -2)
    blocks[-1], blocks[1] = hop(own, 1), hop(own, -1)
    blocks[far] = hop(blocks[-2], 2)
    blocks[-3], blocks[3] = hop(blocks[-2], 1), hop(blocks[2], -1)
    order = sorted(blocks)
    up_mat, down_mat = load([w_up[0], w_down[0]], blocks[-1])
    parts = experts([blocks[q] for q in order], w_gate[0], up_mat, down_mat, tail, order.index(0))
    part = dict(zip(order, parts))
    ahead = plus(part[2], hop(part[far], 2), hop(part[3], 1))
    back = plus(part[-2], hop(part[-3], -1))
    middle = plus(part[0], hop(part[1], 1), hop(part[-1], -1))
    ahead, back = hop(ahead, 2, 1), hop(back, -2, 1)
    carrier = hop(middle, 0, 1)
    expert_out = plus(carrier, ahead, back, width=width)
    returned = lax.all_to_all(
        expert_out.reshape(n_node, CAP, width), "node", split_axis=0, concat_axis=0, tiled=True
    ).reshape(rows_dev, width)
    return combine_rows(carrier, returned, tokens.shape[1])[None]


def solution(mesh):
    placed = (
        P("section", ("node", "local"), None),
        P("section", ("node", "local"), None),
        P("section", ("node", "local"), None),
        P(),
        P("node", None, "local"),
        P("node", None, "local"),
        P("node", "local", None),
    )
    return jax.shard_map(
        shards,
        mesh=mesh,
        in_specs=placed,
        out_specs=P("section", ("node", "local"), None),
        check_vma=False,
    )
```

```python
import jax
import jax.numpy as jnp
from jax import lax
from jax.experimental import pallas as pl
from jax.experimental.pallas import tpu as pltpu
from jax.sharding import PartitionSpec as P

CAP = 2
COLUMNS = 896
PIECE = 1792
LANES = 128
SPLIT = 3
STAGE = 1024
VMEM = pl.BlockSpec(memory_space=pltpu.VMEM)
ANY = pl.BlockSpec(memory_space=pl.ANY)
HBM = pl.BlockSpec(memory_space=pltpu.HBM)


def grant(mib):
    return pltpu.CompilerParams(vmem_limit_bytes=mib * 1024 * 1024)


def cost(flops, moved):
    return pl.CostEstimate(flops=flops, bytes_accessed=moved, transcendentals=0)


def pick_kernel(
    table_ref, routes_hbm, gates_hbm, tokens_hbm, rows_ref, combine_ref, routes_ref, gates_ref, tokens_ref, arrived
):
    slots = table_ref.shape[0]
    rows_dev = combine_ref.shape[0]
    tok_dev, width = tokens_ref.shape
    starts = range(0, width, PIECE)
    small = [
        pltpu.make_async_copy(routes_hbm, routes_ref, arrived.at[0]),
        pltpu.make_async_copy(gates_hbm, gates_ref, arrived.at[1]),
    ]
    pieces = []
    for k, c in enumerate(starts):
        cols = pl.ds(c, min(PIECE, width - c))
        pieces.append(
            pltpu.make_async_copy(tokens_hbm.at[:, cols], tokens_ref.at[:, cols], arrived.at[2 + k])
        )
    for copy in small + pieces:
        copy.start()
    for copy in small:
        copy.wait()
    picks = routes_ref[...]
    gates = gates_ref[...]
    row_slot = lax.broadcasted_iota(jnp.int32, (rows_dev, tok_dev), 0) // CAP
    row_pos = lax.broadcasted_iota(jnp.int32, (rows_dev, tok_dev), 0) % CAP
    named = jnp.zeros((rows_dev, tok_dev), jnp.float32)
    weight = jnp.zeros((rows_dev, tok_dev), jnp.float32)
    want = jnp.zeros((rows_dev, tok_dev), jnp.int32)
    for s in range(slots):
        expert = table_ref[s]
        copies = jnp.int32(0)
        earlier = jnp.int32(0)
        for other in range(slots):
            same = (table_ref[other] == expert).astype(jnp.int32)
            copies = copies + same
            if other < s:
                earlier = earlier + same
        match = picks == expert
        named_s = jnp.sum(match.astype(jnp.float32), axis=0, keepdims=True)
        weight_s = jnp.sum(jnp.where(match, gates, 0.0), axis=0, keepdims=True)
        here = row_slot == s
        named = jnp.where(here, named_s, named)
        weight = jnp.where(here, weight_s, weight)
        want = jnp.where(here, row_pos * copies + earlier, want)
    before = lax.broadcasted_iota(jnp.int32, (tok_dev, tok_dev), 0)
    after = lax.broadcasted_iota(jnp.int32, (tok_dev, tok_dev), 1)
    triangle = (before < after).astype(jnp.float32).astype(jnp.bfloat16)
    rank = jnp.dot(named.astype(jnp.bfloat16), triangle, preferred_element_type=jnp.float32)
    chosen = (named > 0.0) & (rank == want.astype(jnp.float32))
    weight = jnp.where(chosen, weight, 0.0)
    combine_ref[...] = jnp.zeros_like(combine_ref)
    for k in range(SPLIT):
        piece = weight.astype(jnp.bfloat16)
        weight = weight - piece.astype(jnp.float32)
        combine_ref[:, k * LANES : k * LANES + tok_dev] = piece
    select = jnp.where(chosen, 1.0, 0.0).astype(jnp.bfloat16)
    for copy, c in zip(pieces, starts):
        copy.wait()
        cols = slice(c, min(c + PIECE, width))
        rows = jnp.dot(select, tokens_ref[:, cols], preferred_element_type=jnp.float32)
        rows_ref[:, :, cols] = rows.reshape(slots, CAP, rows.shape[1]).astype(jnp.bfloat16)


def pick_rows(table, picks, gates, tokens, rows_dev):
    tok_dev, width = tokens.shape
    return pl.pallas_call(
        pick_kernel,
        out_shape=(
            jax.ShapeDtypeStruct((rows_dev // CAP, CAP, width), jnp.bfloat16),
            jax.ShapeDtypeStruct((rows_dev, SPLIT * LANES), jnp.bfloat16),
        ),
        in_specs=[pl.BlockSpec(memory_space=pltpu.SMEM), HBM, HBM, HBM],
        out_specs=(VMEM, VMEM),
        scratch_shapes=[
            pltpu.VMEM(picks.shape, picks.dtype),
            pltpu.VMEM(gates.shape, gates.dtype),
            pltpu.VMEM(tokens.shape, tokens.dtype),
            pltpu.SemaphoreType.DMA((2 + -(-width // PIECE),)),
        ],
        cost_estimate=cost(2 * rows_dev * tok_dev * width, 2 * (tok_dev + rows_dev) * width),
        name="pick_rows",
    )(table, picks, gates, tokens)


def load_kernel(n, *refs):
    sources, targets, arrived = refs[:n], refs[n + 1 : 2 * n + 1], refs[2 * n + 1]
    copies = [
        pltpu.make_async_copy(source, target, arrived.at[k])
        for k, (source, target) in enumerate(zip(sources, targets))
    ]
    for copy in copies:
        copy.start()
    for copy in copies:
        copy.wait()


def load(arrays, after):
    n = len(arrays)
    return pl.pallas_call(
        lambda *refs: load_kernel(n, *refs),
        out_shape=[jax.ShapeDtypeStruct(a.shape, a.dtype) for a in arrays],
        in_specs=[HBM] * n + [ANY],
        out_specs=[VMEM] * n,
        scratch_shapes=[pltpu.SemaphoreType.DMA((n,))],
        compiler_params=grant(16),
        cost_estimate=cost(1_000_000_000, sum(2 * a.size * a.dtype.itemsize for a in arrays)),
        name="load",
    )(*arrays, after)


def experts_kernel(n, own, *refs):
    blocks, (gate_ref, up_ref, down_ref, tail_ref), outs = refs[:n], refs[n : n + 4], refs[n + 4 :]
    rows_dev, width = blocks[0].shape
    hid = gate_ref.shape[1]
    gate_proj = jnp.zeros((n * rows_dev, hid), jnp.float32)
    up_proj = jnp.zeros((n * rows_dev, hid), jnp.float32)
    for c in range(0, width, COLUMNS):
        cols = slice(c, min(c + COLUMNS, width))
        rows = jnp.concatenate([b[:, cols] for b in blocks], axis=0)
        gate_proj += jnp.dot(rows, gate_ref[cols, :], preferred_element_type=jnp.float32)
        up_proj += jnp.dot(rows, up_ref[cols, :], preferred_element_type=jnp.float32)
    silu = gate_proj / (1.0 + jnp.exp(-gate_proj))
    hidden = (silu * up_proj).astype(jnp.bfloat16)
    for c in range(0, width, COLUMNS):
        cols = slice(c, min(c + COLUMNS, width))
        part = jnp.dot(hidden, down_ref[:, cols], preferred_element_type=jnp.float32)
        part = part.astype(jnp.bfloat16)
        for k in range(n):
            outs[k][:, cols] = part[k * rows_dev : (k + 1) * rows_dev]
    outs[own][:, width:] = tail_ref[...]


def experts(blocks, w_gate, w_up, w_down, tail, own):
    n = len(blocks)
    rows_dev, width = blocks[0].shape
    hid = w_gate.shape[1]
    widths = [width + (tail.shape[1] if k == own else 0) for k in range(n)]
    return pl.pallas_call(
        lambda *refs: experts_kernel(n, own, *refs),
        out_shape=[jax.ShapeDtypeStruct((rows_dev, w), jnp.bfloat16) for w in widths],
        in_specs=[VMEM] * (n + 4),
        out_specs=[VMEM] * n,
        compiler_params=grant(24),
        cost_estimate=cost(6 * n * rows_dev * width * hid, 6 * width * hid),
        name="experts",
    )(*blocks, w_gate, w_up, w_down, tail)


def plus_kernel(*refs):
    out_ref = refs[-1]
    width = min(ref.shape[1] for ref in refs)
    total = refs[0][:, :width].astype(jnp.float32)
    for ref in refs[1:-1]:
        total = total + ref[:, :width].astype(jnp.float32)
    out_ref[:, :width] = total.astype(jnp.bfloat16)
    if out_ref.shape[1] > width:
        out_ref[:, width:] = refs[0][:, width:]


def plus(*terms, width=None):
    shape = (terms[0].shape[0], width or terms[0].shape[1])
    size = shape[0] * shape[1]
    return pl.pallas_call(
        plus_kernel,
        out_shape=jax.ShapeDtypeStruct(shape, jnp.bfloat16),
        in_specs=[VMEM] * len(terms),
        out_specs=VMEM,
        compiler_params=grant(4),
        cost_estimate=cost(len(terms) * size, 2 * (len(terms) + 1) * size),
        name="plus",
    )(*terms)


def combine_kernel(carrier_ref, rows_ref, out_hbm, stage_ref, sent):
    tok_dev, width = stage_ref.shape
    pieces = [
        carrier_ref[:, width + k * LANES : width + k * LANES + tok_dev] for k in range(SPLIT)
    ]
    split = jnp.concatenate(pieces, axis=0)
    copies = []
    for k, c in enumerate(range(0, width, STAGE)):
        cols = slice(c, min(c + STAGE, width))
        rows = jnp.concatenate([rows_ref[:, cols]] * SPLIT, axis=0)
        stage_ref[:, cols] = lax.dot_general(
            split, rows, (((0,), (0,)), ((), ())), preferred_element_type=jnp.float32
        ).astype(jnp.bfloat16)
        span = pl.ds(c, min(STAGE, width - c))
        copies.append(
            pltpu.make_async_copy(stage_ref.at[:, span], out_hbm.at[:, span], sent.at[k])
        )
        copies[-1].start()
    for copy in copies:
        copy.wait()


def combine_rows(carrier, rows, tok_dev):
    rows_dev, width = rows.shape
    return pl.pallas_call(
        combine_kernel,
        out_shape=jax.ShapeDtypeStruct((tok_dev, width), jnp.bfloat16),
        in_specs=[VMEM, VMEM],
        out_specs=ANY,
        scratch_shapes=[
            pltpu.VMEM((tok_dev, width), jnp.bfloat16),
            pltpu.SemaphoreType.DMA((-(-width // STAGE),)),
        ],
        compiler_params=grant(8),
        cost_estimate=cost(6 * rows_dev * tok_dev * width, 2 * (tok_dev + rows_dev) * width),
        name="combine_rows",
    )(carrier, rows)


def hop(block, step, sections=0):
    count = lax.axis_size("section")
    nodes = lax.axis_size("node")
    n = lax.axis_size("local")
    pairs = []
    for s in range(count - sections):
        for node in range(nodes):
            way = step if node % 2 == 0 else -step
            for i in range(n):
                source = (s * nodes + node) * n + i
                pairs.append((source, ((s + sections) * nodes + node) * n + (i + way) % n))
    return lax.ppermute(block, ("section", "node", "local"), pairs)


def shards(tokens, routes, route_gates, replica_table, w_gate, w_up, w_down):
    n_node = lax.axis_size("node")
    far = lax.axis_size("local") // 2
    rows_dev = n_node * CAP
    width = tokens.shape[2]
    outgoing, tail = pick_rows(replica_table, routes[0].T, route_gates[0].T, tokens[0], rows_dev)
    own = lax.all_to_all(outgoing, "node", split_axis=0, concat_axis=0, tiled=True).reshape(
        rows_dev, width
    )
    blocks = {0: own}
    blocks[-2], blocks[2] = hop(own, 2), hop(own, -2)
    blocks[-1], blocks[1] = hop(own, 1), hop(own, -1)
    blocks[far] = hop(blocks[-2], 2)
    blocks[-3], blocks[3] = hop(blocks[-2], 1), hop(blocks[2], -1)
    order = sorted(blocks)
    up_mat, down_mat = load([w_up[0], w_down[0]], blocks[-1])
    parts = experts([blocks[q] for q in order], w_gate[0], up_mat, down_mat, tail, order.index(0))
    part = dict(zip(order, parts))
    ahead = plus(part[2], hop(part[far], 2), hop(part[3], 1))
    back = plus(part[-2], hop(part[-3], -1))
    middle = plus(part[0], hop(part[1], 1), hop(part[-1], -1))
    ahead, back = hop(ahead, 2, 1), hop(back, -2, 1)
    carrier = hop(middle, 0, 1)
    expert_out = plus(carrier, ahead, back, width=width)
    returned = lax.all_to_all(
        expert_out.reshape(n_node, CAP, width), "node", split_axis=0, concat_axis=0, tiled=True
    ).reshape(rows_dev, width)
    return combine_rows(carrier, returned, tokens.shape[1])[None]


def solution(mesh):
    placed = (
        P("section", ("node", "local"), None),
        P("section", ("node", "local"), None),
        P("section", ("node", "local"), None),
        P(),
        P("node", None, "local"),
        P("node", None, "local"),
        P("node", "local", None),
    )
    return jax.shard_map(
        shards,
        mesh=mesh,
        in_specs=placed,
        out_specs=P("section", ("node", "local"), None),
        check_vma=False,
    )
```

```python
import jax
import jax.numpy as jnp
from jax import lax
from jax.experimental import pallas as pl
from jax.experimental.pallas import tpu as pltpu
from jax.sharding import PartitionSpec as P

CAP = 2
COLUMNS = 896
PIECE = 1792
LANES = 128
SPLIT = 3
STAGE = 1024
VMEM = pl.BlockSpec(memory_space=pltpu.VMEM)
ANY = pl.BlockSpec(memory_space=pl.ANY)
HBM = pl.BlockSpec(memory_space=pltpu.HBM)


def grant(mib):
    return pltpu.CompilerParams(vmem_limit_bytes=mib * 1024 * 1024)


def cost(flops, moved):
    return pl.CostEstimate(flops=flops, bytes_accessed=moved, transcendentals=0)


def pick_kernel(
    table_hbm, routes_hbm, gates_hbm, tokens_hbm, rows_hbm, combine_ref,
    table_ref, routes_ref, gates_ref, tokens_ref, rows_ref, arrived, sent,
):
    slots = table_ref.shape[0]
    rows_dev = combine_ref.shape[0]
    tok_dev, width = tokens_ref.shape
    starts = range(0, width, PIECE)
    small = [
        pltpu.make_async_copy(routes_hbm, routes_ref, arrived.at[0]),
        pltpu.make_async_copy(gates_hbm, gates_ref, arrived.at[1]),
        pltpu.make_async_copy(table_hbm, table_ref, arrived.at[2]),
    ]
    pieces = []
    for k, c in enumerate(starts):
        cols = pl.ds(c, min(PIECE, width - c))
        pieces.append(
            pltpu.make_async_copy(tokens_hbm.at[:, cols], tokens_ref.at[:, cols], arrived.at[3 + k])
        )
    for copy in small + pieces:
        copy.start()
    for copy in small:
        copy.wait()
    picks = routes_ref[...]
    gates = gates_ref[...]
    row_slot = lax.broadcasted_iota(jnp.int32, (rows_dev, tok_dev), 0) // CAP
    row_pos = lax.broadcasted_iota(jnp.int32, (rows_dev, tok_dev), 0) % CAP
    named = jnp.zeros((rows_dev, tok_dev), jnp.float32)
    weight = jnp.zeros((rows_dev, tok_dev), jnp.float32)
    want = jnp.zeros((rows_dev, tok_dev), jnp.int32)
    for s in range(slots):
        expert = table_ref[s]
        copies = jnp.int32(0)
        earlier = jnp.int32(0)
        for other in range(slots):
            same = (table_ref[other] == expert).astype(jnp.int32)
            copies = copies + same
            if other < s:
                earlier = earlier + same
        match = picks == expert
        named_s = jnp.sum(match.astype(jnp.float32), axis=0, keepdims=True)
        weight_s = jnp.sum(jnp.where(match, gates, 0.0), axis=0, keepdims=True)
        here = row_slot == s
        named = jnp.where(here, named_s, named)
        weight = jnp.where(here, weight_s, weight)
        want = jnp.where(here, row_pos * copies + earlier, want)
    before = lax.broadcasted_iota(jnp.int32, (tok_dev, tok_dev), 0)
    after = lax.broadcasted_iota(jnp.int32, (tok_dev, tok_dev), 1)
    triangle = (before < after).astype(jnp.float32).astype(jnp.bfloat16)
    rank = jnp.dot(named.astype(jnp.bfloat16), triangle, preferred_element_type=jnp.float32)
    chosen = (named > 0.0) & (rank == want.astype(jnp.float32))
    weight = jnp.where(chosen, weight, 0.0)
    combine_ref[...] = jnp.zeros_like(combine_ref)
    for k in range(SPLIT):
        piece = weight.astype(jnp.bfloat16)
        weight = weight - piece.astype(jnp.float32)
        combine_ref[:, k * LANES : k * LANES + tok_dev] = piece
    select = jnp.where(chosen, 1.0, 0.0).astype(jnp.bfloat16)
    sends = []
    for k, (copy, c) in enumerate(zip(pieces, starts)):
        copy.wait()
        cols = slice(c, min(c + PIECE, width))
        rows = jnp.dot(select, tokens_ref[:, cols], preferred_element_type=jnp.float32)
        rows_ref[:, :, cols] = rows.reshape(slots, CAP, rows.shape[1]).astype(jnp.bfloat16)
        span = pl.ds(c, min(PIECE, width - c))
        sends.append(
            pltpu.make_async_copy(rows_ref.at[:, :, span], rows_hbm.at[:, :, span], sent.at[k])
        )
        sends[-1].start()
    for send in sends:
        send.wait()


def pick_rows(table, picks, gates, tokens, rows_dev):
    tok_dev, width = tokens.shape
    return pl.pallas_call(
        pick_kernel,
        out_shape=(
            jax.ShapeDtypeStruct((rows_dev // CAP, CAP, width), jnp.bfloat16),
            jax.ShapeDtypeStruct((rows_dev, SPLIT * LANES), jnp.bfloat16),
        ),
        in_specs=[HBM, HBM, HBM, HBM],
        out_specs=(HBM, VMEM),
        scratch_shapes=[
            pltpu.SMEM(table.shape, table.dtype),
            pltpu.VMEM(picks.shape, picks.dtype),
            pltpu.VMEM(gates.shape, gates.dtype),
            pltpu.VMEM(tokens.shape, tokens.dtype),
            pltpu.VMEM((rows_dev // CAP, CAP, width), tokens.dtype),
            pltpu.SemaphoreType.DMA((3 + -(-width // PIECE),)),
            pltpu.SemaphoreType.DMA((-(-width // PIECE),)),
        ],
        cost_estimate=cost(2 * rows_dev * tok_dev * width, 2 * (tok_dev + rows_dev) * width),
        name="pick_rows",
    )(table, picks, gates, tokens)


def load_kernel(n, *refs):
    sources, targets, arrived = refs[:n], refs[n + 1 : 2 * n + 1], refs[2 * n + 1]
    copies = [
        pltpu.make_async_copy(source, target, arrived.at[k])
        for k, (source, target) in enumerate(zip(sources, targets))
    ]
    for copy in copies:
        copy.start()
    for copy in copies:
        copy.wait()


def load(arrays, after):
    n = len(arrays)
    return pl.pallas_call(
        lambda *refs: load_kernel(n, *refs),
        out_shape=[jax.ShapeDtypeStruct(a.shape, a.dtype) for a in arrays],
        in_specs=[HBM] * n + [ANY],
        out_specs=[VMEM] * n,
        scratch_shapes=[pltpu.SemaphoreType.DMA((n,))],
        compiler_params=grant(16),
        cost_estimate=cost(1_000_000_000, sum(2 * a.size * a.dtype.itemsize for a in arrays)),
        name="load",
    )(*arrays, after)


def experts_kernel(n, own, *refs):
    blocks, (gate_ref, up_ref, down_ref, tail_ref), outs = refs[:n], refs[n : n + 4], refs[n + 4 :]
    rows_dev, width = blocks[0].shape
    hid = gate_ref.shape[1]
    gate_proj = jnp.zeros((n * rows_dev, hid), jnp.float32)
    up_proj = jnp.zeros((n * rows_dev, hid), jnp.float32)
    for c in range(0, width, COLUMNS):
        cols = slice(c, min(c + COLUMNS, width))
        rows = jnp.concatenate([b[:, cols] for b in blocks], axis=0)
        gate_proj += jnp.dot(rows, gate_ref[cols, :], preferred_element_type=jnp.float32)
        up_proj += jnp.dot(rows, up_ref[cols, :], preferred_element_type=jnp.float32)
    silu = gate_proj / (1.0 + jnp.exp(-gate_proj))
    hidden = (silu * up_proj).astype(jnp.bfloat16)
    for c in range(0, width, COLUMNS):
        cols = slice(c, min(c + COLUMNS, width))
        part = jnp.dot(hidden, down_ref[:, cols], preferred_element_type=jnp.float32)
        part = part.astype(jnp.bfloat16)
        for k in range(n):
            outs[k][:, cols] = part[k * rows_dev : (k + 1) * rows_dev]
    if own is not None:
        outs[own][:, width:] = tail_ref[...]


def experts(blocks, w_gate, w_up, w_down, tail, own):
    n = len(blocks)
    rows_dev, width = blocks[0].shape
    hid = w_gate.shape[1]
    widths = [width + (tail.shape[1] if k == own else 0) for k in range(n)]
    return pl.pallas_call(
        lambda *refs: experts_kernel(n, own, *refs),
        out_shape=[jax.ShapeDtypeStruct((rows_dev, w), jnp.bfloat16) for w in widths],
        in_specs=[VMEM] * (n + 4),
        out_specs=[VMEM] * n,
        compiler_params=grant(24),
        cost_estimate=cost(6 * n * rows_dev * width * hid, 6 * width * hid),
        name="experts",
    )(*blocks, w_gate, w_up, w_down, tail)


def plus_kernel(*refs):
    out_ref = refs[-1]
    width = min(ref.shape[1] for ref in refs)
    total = refs[0][:, :width].astype(jnp.float32)
    for ref in refs[1:-1]:
        total = total + ref[:, :width].astype(jnp.float32)
    out_ref[:, :width] = total.astype(jnp.bfloat16)
    if out_ref.shape[1] > width:
        out_ref[:, width:] = refs[0][:, width:]


def plus(*terms, width=None):
    shape = (terms[0].shape[0], width or terms[0].shape[1])
    size = shape[0] * shape[1]
    return pl.pallas_call(
        plus_kernel,
        out_shape=jax.ShapeDtypeStruct(shape, jnp.bfloat16),
        in_specs=[VMEM] * len(terms),
        out_specs=VMEM,
        compiler_params=grant(4),
        cost_estimate=cost(len(terms) * size, 2 * (len(terms) + 1) * size),
        name="plus",
    )(*terms)


def combine_kernel(carrier_ref, rows_ref, out_hbm, stage_ref, sent):
    tok_dev, width = stage_ref.shape
    pieces = [
        carrier_ref[:, width + k * LANES : width + k * LANES + tok_dev] for k in range(SPLIT)
    ]
    split = jnp.concatenate(pieces, axis=0)
    copies = []
    for k, c in enumerate(range(0, width, STAGE)):
        cols = slice(c, min(c + STAGE, width))
        rows = jnp.concatenate([rows_ref[:, cols]] * SPLIT, axis=0)
        stage_ref[:, cols] = lax.dot_general(
            split, rows, (((0,), (0,)), ((), ())), preferred_element_type=jnp.float32
        ).astype(jnp.bfloat16)
        span = pl.ds(c, min(STAGE, width - c))
        copies.append(
            pltpu.make_async_copy(stage_ref.at[:, span], out_hbm.at[:, span], sent.at[k])
        )
        copies[-1].start()
    for copy in copies:
        copy.wait()


def combine_rows(carrier, rows, tok_dev):
    rows_dev, width = rows.shape
    return pl.pallas_call(
        combine_kernel,
        out_shape=jax.ShapeDtypeStruct((tok_dev, width), jnp.bfloat16),
        in_specs=[VMEM, VMEM],
        out_specs=ANY,
        scratch_shapes=[
            pltpu.VMEM((tok_dev, width), jnp.bfloat16),
            pltpu.SemaphoreType.DMA((-(-width // STAGE),)),
        ],
        compiler_params=grant(8),
        cost_estimate=cost(6 * rows_dev * tok_dev * width, 2 * (tok_dev + rows_dev) * width),
        name="combine_rows",
    )(carrier, rows)


def hop(block, step, sections=0):
    count = lax.axis_size("section")
    nodes = lax.axis_size("node")
    n = lax.axis_size("local")
    pairs = []
    for s in range(count - sections):
        for node in range(nodes):
            way = step if node % 2 == 0 else -step
            for i in range(n):
                source = (s * nodes + node) * n + i
                pairs.append((source, ((s + sections) * nodes + node) * n + (i + way) % n))
    return lax.ppermute(block, ("section", "node", "local"), pairs)


def shards(tokens, routes, route_gates, replica_table, w_gate, w_up, w_down):
    n_node = lax.axis_size("node")
    far = lax.axis_size("local") // 2
    rows_dev = n_node * CAP
    width = tokens.shape[2]
    outgoing, tail = pick_rows(replica_table, routes[0].T, route_gates[0].T, tokens[0], rows_dev)
    own = lax.all_to_all(outgoing, "node", split_axis=0, concat_axis=0, tiled=True).reshape(
        rows_dev, width
    )
    blocks = {0: own}
    blocks[-2], blocks[2] = hop(own, 2), hop(own, -2)
    blocks[-1], blocks[1] = hop(own, 1), hop(own, -1)
    blocks[far] = hop(blocks[-2], 2)
    blocks[-3], blocks[3] = hop(blocks[-2], 1), hop(blocks[2], -1)
    up_mat, down_mat = load([w_up[0], w_down[0]], blocks[-1])
    near, last = [0, -1, 1, -2, 2], [far, -3, 3]
    mats = (w_gate[0], up_mat, down_mat, tail)
    part = dict(zip(near, experts([blocks[q] for q in near], *mats, 0)))
    part.update(zip(last, experts([blocks[q] for q in last], *mats, None)))
    ahead = plus(part[2], hop(part[far], 2), hop(part[3], 1))
    back = plus(part[-2], hop(part[-3], -1))
    middle = plus(part[0], hop(part[1], 1), hop(part[-1], -1))
    ahead, back = hop(ahead, 2, 1), hop(back, -2, 1)
    carrier = hop(middle, 0, 1)
    expert_out = plus(carrier, ahead, back, width=width)
    returned = lax.all_to_all(
        expert_out.reshape(n_node, CAP, width), "node", split_axis=0, concat_axis=0, tiled=True
    ).reshape(rows_dev, width)
    return combine_rows(carrier, returned, tokens.shape[1])[None]


def solution(mesh):
    placed = (
        P("section", ("node", "local"), None),
        P("section", ("node", "local"), None),
        P("section", ("node", "local"), None),
        P(),
        P("node", None, "local"),
        P("node", None, "local"),
        P("node", "local", None),
    )
    return jax.shard_map(
        shards,
        mesh=mesh,
        in_specs=placed,
        out_specs=P("section", ("node", "local"), None),
        check_vma=False,
    )
```
